512 devices in a mesh: gx: 4 (over x), gy: 8 (over y, core), gz: 16 (over z).
Axes of the slice: x: 4, y: 4, z: 16, core: 2. Of those that a mesh axis runs over, the one named last changes fastest.
Arguments:
- output_grad: bfloat16 [524288, 1024], P(('gx', 'gy', 'gz')), may hold values from -6 to 6
- entries: int32 [524288, 32], P(('gx', 'gy', 'gz')), may hold values from 0 to 2047, as said below
- weights: bfloat16 [524288, 32], P(('gx', 'gy', 'gz')), may hold values from 0.0099487305 to 0.099609375
- hot_blocks: int32 [512, 16], P(('gx', 'gy', 'gz')), may hold values from -1 to 63, as said below
- block_counts: int32 [512], P(('gx', 'gy', 'gz')), may hold values from 8 to 16, as said below
- param: float32 [4, 16, 128, 1024], P('gx', 'gz', 'gy'), may hold values from -6 to 6
- first_moment: float32 [4, 16, 128, 1024], P('gx', 'gz', 'gy'), may hold values from -4 to 4
- second_moment: float32 [4, 16, 128, 1024], P('gx', 'gz', 'gy'), may hold values from 0.05 to 1
Outputs:
- new_param: float32 [4, 16, 128, 1024], P('gx', 'gz', 'gy')
- new_first: float32 [4, 16, 128, 1024], P('gx', 'gz', 'gy')
- new_second: float32 [4, 16, 128, 1024], P('gx', 'gz', 'gy')
The draws below stay inside these ranges and needn't reach their ends.
Inputs may be any that keep to these rules, and one draw needn't show every extreme that they name: `hot_blocks`: row d lists device d's hot blocks (block b is rows b * 128 to b * 128 + 127 of the table laid out as 8192 rows) in its first block_counts[d] slots and -1 in the others. The listed blocks of one row differ pairwise modulo 16. Among the devices that differ only in their gz index, some value modulo 16 is listed by every one of them. `block_counts`: among the devices that differ only in their gz index, at least one uses all 16 slots. `entries`: an entry e of a token of device d names a used slot: e // 128 < block_counts[d].
All inputs are finite; a program needn't handle non-finite values.
Results may differ from the reference program's by a relative error of at most 0.00034.
Values sent between devices are 32-bit elements; how exact they have to be, the bound alone decides.
No kernel may reach another device: no remote copies, remote signals or barrier semaphores. Data moves between devices by JAX's collectives and lax.ppermute only.
A program may use at most 128 MiB of HBM per device.

```python
import math
import jax
import jax.numpy as jnp
from jax import lax

D = 1024
BLOCK = 128
KNN = 32
TOK_DEV = 1024
HOT = 16
NBLK = 64
TOKENS = 524288
N_GX = 4
N_GZ = 16
DEVICES = 512


def shuffled_row(row_key):
    return jax.random.permutation(row_key, HOT).astype(jnp.int32)


def hot_lists(key):
    keys = jax.random.split(jax.random.fold_in(key, 5), 8)
    line_count = DEVICES // N_GZ
    device = jnp.arange(DEVICES, dtype=jnp.int32)
    line = device // N_GZ
    position = device % N_GZ
    counts = jax.random.randint(keys[0], (DEVICES,), HOT // 2, HOT + 1, dtype=jnp.int32)
    full_member = jax.random.randint(keys[1], (line_count,), 0, N_GZ, dtype=jnp.int32)
    counts = jnp.where(position == full_member[line], HOT, counts).astype(jnp.int32)
    orders = jax.vmap(shuffled_row)(jax.random.split(keys[2], DEVICES))
    common = jax.random.randint(keys[3], (line_count,), 0, N_GZ, dtype=jnp.int32)[line]
    target = jax.random.randint(keys[4], (DEVICES,), 0, counts, dtype=jnp.int32)
    slot_index = jnp.arange(HOT, dtype=jnp.int32)
    where_now = jnp.argmax(orders == common[:, None], axis=1).astype(jnp.int32)
    at_target = jnp.take_along_axis(orders, target[:, None], axis=1)
    orders = jnp.where(slot_index[None, :] == target[:, None], common[:, None], jnp.where(slot_index[None, :] == where_now[:, None], at_target, orders))
    first_pick = jax.random.randint(keys[5], (DEVICES, HOT), 0, N_GX, dtype=jnp.int32)
    second_pick = jax.random.randint(keys[6], (DEVICES, HOT), 0, N_GX, dtype=jnp.int32)
    offset = jax.random.randint(keys[7], (), 0, N_GX, dtype=jnp.int32)
    column = (jnp.minimum(first_pick, second_pick) + offset) % N_GX
    blocks = jnp.where(slot_index[None, :] < counts[:, None], column * N_GZ + orders, -1)
    return (blocks.astype(jnp.int32), counts)


def draw_hot_blocks(key, part):
    return hot_lists(key)[0]


def draw_block_counts(key, part):
    return hot_lists(key)[1]


def draw_entries(key, part):
    counts = hot_lists(key)[1]
    slot_key, row_key = jax.random.split(jax.random.fold_in(key, 11))
    owner = jnp.arange(TOKENS, dtype=jnp.int32) // TOK_DEV
    slot_pick = jax.random.randint(slot_key, (TOKENS, KNN), 0, counts[owner][:, None], dtype=jnp.int32)
    row_pick = jax.random.randint(row_key, (TOKENS, KNN), 0, BLOCK, dtype=jnp.int32)
    return (slot_pick * BLOCK + row_pick).astype(jnp.int32)


def block_scale(key, dims, cuts, smallest, top_value):
    def one(dim, shards_of):
        draws = jax.random.uniform(jax.random.fold_in(jax.random.fold_in(key, 6), dim), (shards_of,), jnp.float32, smallest / len(cuts), top_value / len(cuts))
        return jnp.repeat(jnp.exp(draws), dims[dim] // shards_of).reshape((-1,) + (1,) * (len(dims) - dim - 1))

    gain = one(*cuts[0])
    for cut in cuts[1:]:
        gain = gain * one(*cut)
    return gain


def bell_draw(rng, extent, scale, limit, cuts=(), kind=jnp.bfloat16):
    result = jax.random.normal(rng, extent, jnp.float32) * scale
    if len(cuts) > 0:
        result = block_scale(rng, extent, cuts, -0.22, 0.18) * result
    return jnp.clip(result, min=-limit, max=limit).astype(kind)


def setup_inputs(seed: int = 0) -> dict:
    arg_keys = jax.random.split(jax.random.key(seed), 9)
    output_grad = bell_draw(arg_keys[0], (TOKENS, D), 1.0, 6.0, ((0, 512),))
    entries = draw_entries(jax.random.fold_in(arg_keys[8], 71), 0)
    weights = jnp.clip(0.0099487305 + 0.089660645 * jax.random.uniform(arg_keys[2], (TOKENS, KNN), jnp.float32) ** block_scale(arg_keys[2], (TOKENS, KNN), ((0, 512),), -0.2, 0.2), 0.0099487305, 0.099609375).astype(jnp.bfloat16)
    hot_blocks = draw_hot_blocks(jax.random.fold_in(arg_keys[8], 71), 0)
    block_counts = draw_block_counts(jax.random.fold_in(arg_keys[8], 71), 0)
    param = bell_draw(arg_keys[5], (N_GX, N_GZ, BLOCK, D), 1.0, 6.0, ((0, 4), (1, 16), (2, 8)), jnp.float32)
    first_moment = bell_draw(arg_keys[6], (N_GX, N_GZ, BLOCK, D), 0.5, 4.0, ((0, 4), (1, 16), (2, 8)), jnp.float32)
    second_moment = jnp.clip(jnp.exp(math.log(1.0) - 2.9957323 * jax.random.uniform(arg_keys[7], (N_GX, N_GZ, BLOCK, D), jnp.float32) ** block_scale(arg_keys[7], (N_GX, N_GZ, BLOCK, D), ((0, 4), (1, 16), (2, 8)), -0.2, 0.2)), 0.05, 1.0)
    return dict(output_grad=output_grad, entries=entries, weights=weights, hot_blocks=hot_blocks, block_counts=block_counts, param=param, first_moment=first_moment, second_moment=second_moment)


first_decay = 0.9
second_decay = 0.99
learning_rate = 0.01
adam_epsilon = 1e-08
first_debias = 1.0 / (1.0 - 0.9 ** 10)
second_debias = 1.0 / (1.0 - 0.99 ** 10)

def reference(output_grad, entries, weights, hot_blocks, block_counts, param, first_moment, second_moment):
    slot_index = jnp.arange(HOT, dtype=jnp.int32)
    token_index = jnp.arange(TOK_DEV, dtype=jnp.int32)[:, None]

    def device_step(device, totals):
        start = (device * TOK_DEV).astype(jnp.int32)
        grads = lax.dynamic_slice_in_dim(output_grad, start, TOK_DEV, 0)
        picks = lax.dynamic_slice_in_dim(entries, start, TOK_DEV, 0).astype(jnp.int32)
        scales = lax.dynamic_slice_in_dim(weights, start, TOK_DEV, 0)
        listed = lax.dynamic_index_in_dim(hot_blocks, device, 0, keepdims=False).astype(jnp.int32)
        used = lax.dynamic_index_in_dim(block_counts, device, 0, keepdims=False).astype(jnp.int32)
        flat_index = (picks * TOK_DEV + token_index).reshape(-1)
        spread = jnp.zeros((HOT * BLOCK * TOK_DEV,), jnp.float32).at[flat_index].add(scales.astype(jnp.float32).reshape(-1))
        spread = spread.reshape(HOT * BLOCK, TOK_DEV).astype(jnp.bfloat16)
        partial_value = jnp.dot(spread, grads, preferred_element_type=jnp.float32)
        usable = (slot_index < used) & (listed >= 0)
        target = jnp.where(usable, listed, NBLK).astype(jnp.int32)
        return totals.at[target].add(partial_value.reshape(HOT, BLOCK, D), mode='drop')
    totals = lax.fori_loop(0, DEVICES, device_step, jnp.zeros((NBLK, BLOCK, D), jnp.float32))
    gradient = totals.reshape(N_GX, N_GZ, BLOCK, D)
    new_first = first_decay * first_moment + (1.0 - first_decay) * gradient
    new_second = second_decay * second_moment + (1.0 - second_decay) * gradient * gradient
    new_param = param - learning_rate * (new_first * first_debias) / (jnp.sqrt(new_second * second_debias) + adam_epsilon)
    return (new_param, new_first, new_second)
```

```python
import jax
import jax.numpy as jnp
from jax import lax
from jax.experimental import pallas as pl
from jax.experimental.pallas import tpu as pltpu
from jax.sharding import PartitionSpec as P

BLOCK = 128
F32 = jnp.float32
BF16 = jnp.bfloat16

first_decay = 0.9
second_decay = 0.99
learning_rate = 0.01
adam_epsilon = 1e-08
first_debias = 1.0 / (1.0 - 0.9**10)
second_debias = 1.0 / (1.0 - 0.99**10)


def spread_body(ent_ref, wgt_ref, out_ref):
    groups = ent_ref.shape[1]
    sub = lax.broadcasted_iota(jnp.int32, (128, 256), 0)
    tok = lax.broadcasted_iota(jnp.int32, (1, 256), 1) // 32

    def pair(p, carry):
        halves = []
        for h in range(2):
            ent = ent_ref[0, pl.ds(2 * p + h, 1), :]
            wgt = wgt_ref[0, pl.ds(2 * p + h, 1), :]
            row = ent & (BLOCK - 1)
            key = (ent >> 7) * 8 + tok
            rows = jnp.where(sub == row, 1.0, 0.0).astype(BF16)
            keys = jnp.where(sub == key, wgt, 0.0).astype(BF16)
            one = lax.dot_general(
                keys, rows, (((1,), (1,)), ((), ())), preferred_element_type=F32
            )
            halves.append(one.reshape(16, 8, BLOCK))
        both = jnp.concatenate(halves, axis=1).astype(BF16)
        start = pl.multiple_of(p * 16, 16)
        for b in range(16):
            out_ref[0, pl.ds(start, 16), b * BLOCK : (b + 1) * BLOCK] = both[b]
        return carry

    lax.fori_loop(0, groups // 2, pair, 0, unroll=4)


def spread_of(entries, weights):
    sources, groups, lanes = entries.shape
    step = 32
    return pl.pallas_call(
        spread_body,
        grid=(sources, groups // step),
        in_specs=[
            pl.BlockSpec((1, step, lanes), lambda s, i: (s, i, 0)),
            pl.BlockSpec((1, step, lanes), lambda s, i: (s, i, 0)),
        ],
        out_specs=pl.BlockSpec((1, step * 8, 2048), lambda s, i: (s, i, 0)),
        out_shape=jax.ShapeDtypeStruct((sources, groups * 8, 2048), BF16),
        cost_estimate=pl.CostEstimate(
            flops=sources * groups * 2 * 128 * 256 * 128 * 4,
            bytes_accessed=sources * groups * 8 * 4096,
            transcendentals=0,
        ),
        name="spread",
    )(entries, weights)


def merge_body(col_ref, grad_ref, spread_ref, own_ref, send_ref):
    s = pl.program_id(0)

    @pl.when(s == 0)
    def _():
        own_ref[...] = jnp.zeros_like(own_ref)
        send_ref[...] = jnp.zeros_like(send_ref)

    grad = grad_ref[0].astype(BF16)

    def pair(p, carry):
        start = pl.multiple_of(p * 256, 256)
        part = lax.dot_general(
            spread_ref[0, :, pl.ds(start, 256)],
            grad,
            (((0,), (0,)), ((), ())),
            preferred_element_type=F32,
        )
        for h in range(2):
            bucket = 2 * p + h
            place = (bucket & 3) * 4 + (bucket >> 2)
            col = col_ref[s, bucket]
            for y in range(4):
                at = h * 128 + y * 32
                own_ref[y, place, col] += part[at : at + 16]
                send_ref[y, place, col] += part[at + 16 : at + 32]
        return carry

    lax.fori_loop(0, 8, pair, 0)


def merge(cols, grads, spreads):
    sources, tokens, width = grads.shape
    dense = jax.ShapeDtypeStruct((4, 16, 4, 16, width), F32)
    block = pl.BlockSpec((4, 16, 4, 16, width), lambda s, c: (0, 0, 0, 0, 0))
    return pl.pallas_call(
        merge_body,
        grid_spec=pltpu.PrefetchScalarGridSpec(
            num_scalar_prefetch=1,
            grid=(sources,),
            in_specs=[
                pl.BlockSpec((1, tokens, width), lambda s, c: (s, 0, 0)),
                pl.BlockSpec((1, tokens, 2048), lambda s, c: (s, 0, 0)),
            ],
            out_specs=[block, block],
        ),
        out_shape=[dense, dense],
        cost_estimate=pl.CostEstimate(
            flops=sources * 2 * 2048 * tokens * width,
            bytes_accessed=sources * tokens * (4096 + 4 * width) + 2**23,
            transcendentals=0,
        ),
        name="merge",
    )(cols, grads, spreads)


def adam_update(gradient, param, first_moment, second_moment):
    new_first = first_decay * first_moment + (1.0 - first_decay) * gradient
    new_second = second_decay * second_moment + (1.0 - second_decay) * gradient * gradient
    new_param = param - learning_rate * (new_first * first_debias) / (
        jnp.sqrt(new_second * second_debias) + adam_epsilon
    )
    return (new_param, new_first, new_second)


def shards(
    output_grad, entries, weights, hot_blocks, block_counts, param, first_moment, second_moment
):
    tokens, width = output_grad.shape
    core = lax.axis_index("gy") % 2
    listed = hot_blocks[0]
    slots = jnp.arange(16, dtype=jnp.int32)
    usable = (slots < block_counts[0]) & (listed >= 0)
    safe = jnp.maximum(listed, 0)
    slot_bucket = safe % 16
    hit = (slot_bucket[None, :] == slots[:, None]) & usable[None, :]
    cols = jnp.sum(jnp.where(hit, (safe // 16)[None, :], 0), axis=1)

    match = (entries >> 7)[:, :, None] == slots
    bucket = jnp.sum(jnp.where(match, slot_bucket, 0), axis=2)
    kept = jnp.any(match & usable, axis=2)
    code = bucket * BLOCK + ((entries & (BLOCK - 1)) ^ (core * 16))
    kept_weights = jnp.where(kept, weights.astype(F32), 0.0)
    small = jnp.concatenate(
        [
            code.astype(F32).reshape(128, 256),
            kept_weights.reshape(128, 256),
            jnp.broadcast_to(jnp.pad(cols.astype(F32), (0, 240))[None], (8, 256)),
        ],
        axis=0,
    )
    small = lax.all_to_all(jnp.broadcast_to(small[None], (4, 264, 256)), "gx", 0, 0, tiled=True)
    wide = jnp.swapaxes(output_grad.astype(F32).reshape(tokens, 4, width // 4), 0, 1)
    grads = lax.all_to_all(wide, "gx", 0, 0, tiled=True)

    spreads = spread_of(small[:, :128].astype(jnp.int32), small[:, 128:256])
    col_table = small[:, 256, :16].astype(jnp.int32)
    own, send = merge(col_table, grads, spreads)
    got = lax.ppermute(send, "gy", [(i, i ^ 1) for i in range(8)])
    chip = own + got
    rows = lax.all_to_all(
        chip, "gy", 0, 0, axis_index_groups=[[0, 2, 4, 6], [1, 3, 5, 7]], tiled=True
    )
    rows = jnp.sum(rows, axis=0)
    near = lax.all_to_all(
        rows.reshape(4, 4, 4, 16, width // 4),
        "gz",
        0,
        0,
        axis_index_groups=[[4 * h + i for i in range(4)] for h in range(4)],
        tiled=True,
    )
    near = jnp.sum(near, axis=0)
    far = lax.all_to_all(
        near.reshape(16, 16, width // 4),
        ("gx", "gz"),
        0,
        0,
        axis_index_groups=[
            [x * 16 + 4 * h + i for h in range(4) for x in range(4)] for i in range(4)
        ],
        tiled=True,
    )
    far = jnp.sum(far.reshape(4, 4, 16, width // 4), axis=0)
    gradient = jnp.swapaxes(far, 0, 1).reshape(param.shape)
    return adam_update(gradient, param, first_moment, second_moment)


def solution(mesh):
    placed = (
        P(("gx", "gy", "gz"), None),
        P(("gx", "gy", "gz"), None),
        P(("gx", "gy", "gz"), None),
        P(("gx", "gy", "gz"), None),
        P(("gx", "gy", "gz")),
        P("gx", "gz", "gy", None),
        P("gx", "gz", "gy", None),
        P("gx", "gz", "gy", None),
    )
    return jax.shard_map(
        shards,
        mesh=mesh,
        in_specs=placed,
        out_specs=(P("gx", "gz", "gy", None), P("gx", "gz", "gy", None), P("gx", "gz", "gy", None)),
        check_vma=False,
    )
```

```python
import jax
import jax.numpy as jnp
from jax import lax
from jax.experimental import pallas as pl
from jax.experimental.pallas import tpu as pltpu
from jax.sharding import PartitionSpec as P


BLOCK = 128
F32 = jnp.float32
BF16 = jnp.bfloat16

first_decay = 0.9
second_decay = 0.99
learning_rate = 0.01
adam_epsilon = 1e-08
first_debias = 1.0 / (1.0 - 0.9**10)
second_debias = 1.0 / (1.0 - 0.99**10)


def widen_body(grad_ref, first_ref, second_ref):
    wide = grad_ref[...].astype(F32)
    first_ref[0] = wide[:, :128]
    second_ref[0] = wide[:, 128:]


def widen(grads):
    tokens, width = grads.shape
    chunk = jax.ShapeDtypeStruct((4, tokens, width // 8), F32)
    spec = pl.BlockSpec((1, tokens, width // 8), lambda x: (x, 0, 0))
    return pl.pallas_call(
        widen_body,
        grid=(4,),
        in_specs=[pl.BlockSpec((tokens, width // 4), lambda x: (0, x))],
        out_specs=[spec, spec],
        out_shape=[chunk, chunk],
        cost_estimate=pl.CostEstimate(flops=2**23, bytes_accessed=6 * 2**20, transcendentals=0),
        name="widen",
    )(grads)


def spread_body(code_ref, wgt_ref, out_ref, turned_ref):
    sub = lax.broadcasted_iota(jnp.int32, (128, 256), 0)
    tok = lax.broadcasted_iota(jnp.int32, (1, 256), 1) // 32

    def pair(p, carry):
        halves = []
        for h in range(2):
            code = code_ref[0, pl.ds(2 * p + h, 1), :].astype(jnp.int32)
            wgt = wgt_ref[0, pl.ds(2 * p + h, 1), :]
            row = code & (BLOCK - 1)
            key = (code >> 7) * 8 + tok
            rows = jnp.where(sub == row, 1.0, 0.0).astype(BF16)
            keys = jnp.where(sub == key, wgt, 0.0).astype(BF16)
            one = lax.dot_general(
                keys, rows, (((1,), (1,)), ((), ())), preferred_element_type=F32
            )
            halves.append(one.reshape(16, 8, BLOCK))
        both = jnp.concatenate(halves, axis=1).astype(BF16)
        start = pl.multiple_of(p * 16, 16)
        for b in range(16):
            turned_ref[b, pl.ds(start, 16), :] = both[b]
        return carry

    lax.fori_loop(0, 8, pair, 0, unroll=4)
    for b in range(16):
        out_ref[0, b * BLOCK : (b + 1) * BLOCK, :] = turned_ref[b].T


def spread_of(small):
    sources = small.shape[0]
    return pl.pallas_call(
        spread_body,
        grid=(sources, 8),
        in_specs=[
            pl.BlockSpec((1, 16, 256), lambda s, i: (s, i, 0)),
            pl.BlockSpec((1, 16, 256), lambda s, i: (s, i + 8, 0)),
        ],
        out_specs=pl.BlockSpec((1, 2048, 128), lambda s, i: (s, 0, i)),
        out_shape=jax.ShapeDtypeStruct((sources, 2048, 1024), BF16),
        scratch_shapes=[pltpu.VMEM((16, 128, BLOCK), BF16)],
        cost_estimate=pl.CostEstimate(
            flops=sources * 2**32, bytes_accessed=sources * 2**22, transcendentals=0
        ),
        name="spread",
    )(small, small)


def merge_body(place_ref, grad_ref, spread_ref, own_ref, send_ref):
    s = pl.program_id(0)

    @pl.when(s == 0)
    def _():
        own_ref[...] = jnp.zeros_like(own_ref)
        send_ref[...] = jnp.zeros_like(send_ref)

    grad = grad_ref[0].astype(BF16)

    def pair(p, carry):
        start = pl.multiple_of(p * 256, 256)
        part = jnp.dot(
            spread_ref[0, pl.ds(start, 256), :], grad, preferred_element_type=F32
        )
        for h in range(2):
            place = place_ref[s, 2 * p + h]

            @pl.when(place >= 0)
            def _():
                side, at = place >> 5, place & 31
                for y in range(4):
                    r = h * 128 + y * 32
                    own_ref[side, y, at] += part[r : r + 16]
                    send_ref[side, y, at] += part[r + 16 : r + 32]

        return carry

    lax.fori_loop(0, 8, pair, 0)


def merge(places, grads, spreads):
    sources, tokens, width = grads.shape
    dense = jax.ShapeDtypeStruct((2, 4, 32, 16, width), F32)
    block = pl.BlockSpec((2, 4, 32, 16, width), lambda s, c: (0, 0, 0, 0, 0))
    return pl.pallas_call(
        merge_body,
        grid_spec=pltpu.PrefetchScalarGridSpec(
            num_scalar_prefetch=1,
            grid=(sources,),
            in_specs=[
                pl.BlockSpec((1, tokens, width), lambda s, c: (s, 0, 0)),
                pl.BlockSpec((1, 2048, tokens), lambda s, c: (s, 0, 0)),
            ],
            out_specs=[block, block],
        ),
        out_shape=[dense, dense],
        cost_estimate=pl.CostEstimate(
            flops=sources * 2 * 2048 * tokens * width,
            bytes_accessed=sources * tokens * (4096 + 4 * width) + 2**22,
            transcendentals=0,
        ),
        name="merge",
    )(places, grads, spreads)


def adam_update(gradient, param, first_moment, second_moment):
    new_first = first_decay * first_moment + (1.0 - first_decay) * gradient
    new_second = second_decay * second_moment + (1.0 - second_decay) * gradient * gradient
    new_param = param - learning_rate * (new_first * first_debias) / (
        jnp.sqrt(new_second * second_debias) + adam_epsilon
    )
    return (new_param, new_first, new_second)


def flip(x, axis, bits):
    size = lax.axis_size(axis)
    return lax.ppermute(x, axis, [(i, i ^ bits) for i in range(size)])


def other_neighbour(x):
    return lax.ppermute(x, "gz", [(i, (((i + 1) ^ 1) - 1) % 16) for i in range(16)])


def to_chip(own, send):
    got = flip(send, "gy", 1)
    low = own[1, :, :16] + got[1, :, :16]
    high = own[1, :, 16:] + got[1, :, 16:]
    return own, got, low, high


def to_owners(own, got, low, high):
    width = own.shape[-1]
    near = [flip(low, "gz", 1), other_neighbour(high)]

    def kept(y):
        near_rows = jnp.concatenate([near[0][y], near[1][y]], axis=0)
        return own[0, y] + got[0, y] + near_rows

    rows = kept(0)
    for piece in [flip(kept(y), "gy", 2 * y) for y in (1, 3, 2)]:
        rows = rows + piece
    far = lax.all_to_all(
        rows,
        ("gx", "gz"),
        0,
        0,
        axis_index_groups=[
            [
                (2 * half + low) * 16 + 2 * u + i
                for half in range(2)
                for u in range(8)
                for low in range(2)
            ]
            for i in range(2)
        ],
        tiled=True,
    )
    far = jnp.sum(far.reshape(2, 8, 2, 16, width), axis=1)
    return far.reshape(4, 16, width)


def shards(
    output_grad, entries, weights, hot_blocks, block_counts, param, first_moment, second_moment
):
    gy = lax.axis_index("gy")
    gz = lax.axis_index("gz")
    listed = hot_blocks[0]
    slots = jnp.arange(16, dtype=jnp.int32)
    usable = (slots < block_counts[0]) & (listed >= 0)
    blocks = jnp.where(usable, listed, -1).astype(F32)

    code = (entries ^ (gy * 16)).astype(F32)
    small = jnp.concatenate(
        [
            code.reshape(128, 256),
            weights.astype(F32).reshape(128, 256),
            jnp.broadcast_to(jnp.pad(blocks, (0, 240))[None], (8, 256)),
        ],
        axis=0,
    )
    small = lax.all_to_all(
        jnp.broadcast_to(small[None], (4, 264, 256)), "gx", 0, 0, tiled=True
    )
    spreads = spread_of(small)
    blocks = small[:, 256, :16].astype(jnp.int32)
    bucket = blocks & 15
    column = blocks >> 4
    side = (bucket ^ gz) & 1
    places = side * 32 + (column >> 1) * 16 + (bucket >> 1) * 2 + (column & 1)
    places = jnp.where(blocks >= 0, places, -1)

    first, second = widen(output_grad)
    first = lax.all_to_all(first, "gx", 0, 0, tiled=True)
    second, spreads = lax.optimization_barrier((second, spreads))
    second = lax.all_to_all(second, "gx", 0, 0, tiled=True)
    first = merge(places, first, spreads)
    own, got, low, high = to_chip(*first)
    second, low, high = lax.optimization_barrier((second, low, high))
    second = merge(places, second, spreads)
    pieces = [to_owners(own, got, low, high), to_owners(*to_chip(*second))]
    gradient = jnp.stack(pieces, axis=1)
    gradient = jnp.moveaxis(gradient, 2, 0).reshape(param.shape)
    return adam_update(gradient, param, first_moment, second_moment)


def solution(mesh):
    placed = (
        P(("gx", "gy", "gz"), None),
        P(("gx", "gy", "gz"), None),
        P(("gx", "gy", "gz"), None),
        P(("gx", "gy", "gz"), None),
        P(("gx", "gy", "gz")),
        P("gx", "gz", "gy", None),
        P("gx", "gz", "gy", None),
        P("gx", "gz", "gy", None),
    )

    return jax.shard_map(
        shards,
        mesh=mesh,
        in_specs=placed,
        out_specs=(P("gx", "gz", "gy", None), P("gx", "gz", "gy", None), P("gx", "gz", "gy", None)),
        check_vma=False,
    )
```
